16 devices in a mesh: dp: 2 (over y, z), sp: 8 (over x, core).
Axes of the slice: x: 4, y: 2, z: 1, core: 2. Of those that a mesh axis runs over, the one named last changes fastest.
The devices are a block of a 4x4x8 slice.
Arguments:
- x: bfloat16 [4096, 2048], P(('dp', 'sp')), parts along dimension 0
- doc_start: int32 [4096], P(('dp', 'sp')), parts along dimension 0
- w_in: bfloat16 [2048, 8384], replicated
- conv_w: float32 [4, 4224], replicated
- conv_b: float32 [4224], replicated
- dt_bias: float32 [64], replicated
- a_log: float32 [64], replicated
- d_skip: float32 [64], replicated
- norm_w: float32 [1, 4096], replicated
- w_out: bfloat16 [4096, 2048], replicated
Outputs:
- output: bfloat16 [4096, 2048], P(('dp', 'sp')), parts along dimension 0
There are 2 independent parts. The reference program is written for one: setup_inputs(seed, part) draws one part's arguments, and reference() takes and returns one part's arrays. A program takes and returns all parts, laid end to end along the dimension named above; an argument that names none is the same for every part.
All inputs are finite; a program needn't handle non-finite values.
Results may differ from the reference program's by a relative error of at most 0.00405549.
Values are sent between devices in bfloat16 or wider.
A program may use at most 768 MiB of HBM per device.

```python
import jax
import jax.numpy as jnp
from jax import lax

SEQ_LEN = 2048
SHARD_LEN = 256
D_MODEL = 2048
NUM_HEADS = 64
HEAD_DIM = 64
NUM_GROUPS = 1
STATE_DIM = 64
CHUNK_LEN = 256
CONV_WIDTH = 4
NORM_EPS = 1e-5
D_INNER = NUM_HEADS * HEAD_DIM
GROUP_WIDTH = D_INNER // NUM_GROUPS
PER_GROUP = NUM_HEADS // NUM_GROUPS
CONV_DIM = D_INNER + 2 * NUM_GROUPS * STATE_DIM
PROJ_DIM = 2 * D_INNER + 2 * NUM_GROUPS * STATE_DIM + NUM_HEADS
N_CHUNKS = SEQ_LEN // CHUNK_LEN
N_SHARDS = SEQ_LEN // SHARD_LEN


def draw_starts(start_key):
    level_key, pos_key = jax.random.split(start_key)
    shard_level = jax.random.randint(level_key, (N_SHARDS, 1), 0, 4)
    pos_draws = jax.random.randint(pos_key, (N_SHARDS, SHARD_LEN), 0, SHARD_LEN)
    return (pos_draws < shard_level).astype(jnp.int32).reshape(SEQ_LEN)


def setup_inputs(seed: int = 0, part: int = 0) -> dict:
    root_key = jax.random.key(seed)
    part_key = jax.random.fold_in(root_key, part)
    x_key, start_key = jax.random.split(part_key)
    weight_keys = jax.random.split(root_key, 8)
    x = jax.random.normal(x_key, (SEQ_LEN, D_MODEL), jnp.float32).astype(jnp.bfloat16)
    doc_start = draw_starts(start_key)
    w_in = (jax.random.normal(weight_keys[0], (D_MODEL, PROJ_DIM), jnp.float32) * D_MODEL ** -0.5).astype(jnp.bfloat16)
    conv_w = jax.random.normal(weight_keys[1], (CONV_WIDTH, CONV_DIM), jnp.float32) * 0.5
    conv_b = jax.random.normal(weight_keys[2], (CONV_DIM,), jnp.float32) * 0.5
    dt_bias = jax.random.uniform(weight_keys[3], (NUM_HEADS,), jnp.float32, -3.5, -2.5)
    decay_rate = jax.random.uniform(weight_keys[4], (NUM_HEADS,), jnp.float32, 0.3, 1.5)
    a_log = jnp.log(decay_rate) - jnp.log(0.08 * SHARD_LEN)
    d_skip = jax.random.uniform(weight_keys[5], (NUM_HEADS,), jnp.float32, 0.5, 1.5)
    norm_w = jax.random.uniform(weight_keys[6], (NUM_GROUPS, GROUP_WIDTH), jnp.float32, 0.5, 1.5)
    w_out = (jax.random.normal(weight_keys[7], (D_INNER, D_MODEL), jnp.float32) * D_INNER ** -0.5).astype(jnp.bfloat16)
    return {'x': x, 'doc_start': doc_start, 'w_in': w_in, 'conv_w': conv_w, 'conv_b': conv_b, 'dt_bias': dt_bias, 'a_log': a_log, 'd_skip': d_skip, 'norm_w': norm_w, 'w_out': w_out}


def chunk_step(run_state, chunk_in):
    xs_blk, b_blk, c_blk, dt_blk, ld_blk, start_blk = chunk_in
    cum_decay = jnp.cumsum(ld_blk, axis=0)
    seg_ids = jnp.cumsum(start_blk)
    position = jnp.arange(CHUNK_LEN)
    allowed = (position[:, None] >= position[None, :]) & (seg_ids[:, None] == seg_ids[None, :])
    cum_rows = jnp.moveaxis(cum_decay, 0, -1)
    decay_mat = jnp.exp(jnp.where(allowed, cum_rows[..., :, None] - cum_rows[..., None, :], -jnp.inf))
    scores = jnp.einsum('ign,jgn->gij', c_blk.astype(jnp.float32), b_blk.astype(jnp.float32))
    mix_mat = (scores[:, None] * decay_mat * jnp.moveaxis(dt_blk, 0, -1)[..., None, :]).astype(jnp.bfloat16)
    y_intra = jnp.einsum('gkij,jgkp->igkp', mix_mat.astype(jnp.float32), xs_blk.astype(jnp.float32))
    w_start = jnp.exp(cum_decay) * (seg_ids == 0)[:, None, None]
    y_state = jnp.einsum('ign,gkpn->igkp', c_blk.astype(jnp.float32), run_state.astype(jnp.bfloat16).astype(jnp.float32)) * w_start[..., None]
    last_cum = cum_decay[-1]
    w_end = jnp.exp(last_cum - cum_decay) * dt_blk * (seg_ids == seg_ids[-1])[:, None, None]
    scaled_x = (xs_blk.astype(jnp.float32) * w_end[..., None]).astype(jnp.bfloat16)
    chunk_state = jnp.einsum('jgkp,jgn->gkpn', scaled_x.astype(jnp.float32), b_blk.astype(jnp.float32))
    next_state = (jnp.exp(last_cum) * (seg_ids[-1] == 0))[..., None, None] * run_state + chunk_state
    return next_state, y_intra + y_state


def reference(x, doc_start, w_in, conv_w, conv_b, dt_bias, a_log, d_skip, norm_w, w_out):
    projected = jnp.dot(x, w_in, preferred_element_type=jnp.float32).astype(jnp.bfloat16)
    gate_in = projected[:, :D_INNER].astype(jnp.float32)
    conv_in = projected[:, D_INNER:D_INNER + CONV_DIM].astype(jnp.float32)
    dt_raw = projected[:, D_INNER + CONV_DIM:].astype(jnp.float32)
    keep_flag = (1 - doc_start).astype(jnp.float32)
    keep_pad = jnp.concatenate([jnp.ones((CONV_WIDTH - 1,), jnp.float32), keep_flag])
    conv_pad = jnp.concatenate([jnp.zeros((CONV_WIDTH - 1, CONV_DIM), jnp.float32), conv_in])
    pre_act = conv_b + conv_w[0] * conv_in
    tap_mask = jnp.ones((SEQ_LEN,), jnp.float32)
    for offset in range(1, CONV_WIDTH):
        tap_mask = tap_mask * keep_pad[CONV_WIDTH - offset:CONV_WIDTH - offset + SEQ_LEN]
        pre_act = pre_act + conv_w[offset] * tap_mask[:, None] * conv_pad[CONV_WIDTH - 1 - offset:CONV_WIDTH - 1 - offset + SEQ_LEN]
    conv_out = jax.nn.silu(pre_act).astype(jnp.bfloat16)
    xs_heads = conv_out[:, :D_INNER]
    b_mat = conv_out[:, D_INNER:D_INNER + NUM_GROUPS * STATE_DIM]
    c_mat = conv_out[:, D_INNER + NUM_GROUPS * STATE_DIM:]
    dt_val = jax.nn.softplus(dt_raw + dt_bias)
    log_decay = -jnp.exp(a_log) * dt_val
    chunk_inputs = (
        xs_heads.reshape(N_CHUNKS, CHUNK_LEN, NUM_GROUPS, PER_GROUP, HEAD_DIM),
        b_mat.reshape(N_CHUNKS, CHUNK_LEN, NUM_GROUPS, STATE_DIM),
        c_mat.reshape(N_CHUNKS, CHUNK_LEN, NUM_GROUPS, STATE_DIM),
        dt_val.reshape(N_CHUNKS, CHUNK_LEN, NUM_GROUPS, PER_GROUP),
        log_decay.reshape(N_CHUNKS, CHUNK_LEN, NUM_GROUPS, PER_GROUP),
        doc_start.reshape(N_CHUNKS, CHUNK_LEN),
    )
    zero_state = jnp.zeros((NUM_GROUPS, PER_GROUP, HEAD_DIM, STATE_DIM), jnp.float32)
    scan_out = lax.scan(chunk_step, zero_state, chunk_inputs)
    y_heads = scan_out[1].reshape(SEQ_LEN, NUM_HEADS, HEAD_DIM) + d_skip[:, None] * xs_heads.reshape(SEQ_LEN, NUM_HEADS, HEAD_DIM).astype(jnp.float32)
    gated_y = y_heads.reshape(SEQ_LEN, NUM_GROUPS, GROUP_WIDTH) * jax.nn.silu(gate_in).reshape(SEQ_LEN, NUM_GROUPS, GROUP_WIDTH)
    normed = gated_y * lax.rsqrt(jnp.mean(gated_y * gated_y, axis=-1, keepdims=True) + NORM_EPS) * norm_w
    return jnp.dot(normed.reshape(SEQ_LEN, D_INNER).astype(jnp.bfloat16), w_out, preferred_element_type=jnp.float32).astype(jnp.bfloat16)
```

```python
import functools
import jax
import jax.numpy as jnp
from jax import lax
from jax.experimental import pallas as pl
from jax.experimental.pallas import tpu as pltpu
from jax.sharding import PartitionSpec as P

NORM_EPS = 1e-5
LOG2E = 1.4426950408889634
F32 = jnp.float32
BF16 = jnp.bfloat16
LANES = 128
HALO = 16
TILE = 512
RING = 6
MESH = pl.DeviceIdType.MESH


def dot(lhs, rhs):
    return jnp.dot(lhs, rhs, preferred_element_type=F32)


def iota(shape, axis):
    return lax.broadcasted_iota(jnp.int32, shape, axis)


def split3(val):
    hi = val.astype(BF16)
    rest = val - hi.astype(F32)
    mid = rest.astype(BF16)
    low = (rest - mid.astype(F32)).astype(BF16)
    return hi, mid, low


def pack3(val):
    hi, mid, low = split3(val)
    first = hi.astype(F32) + pltpu.roll(mid.astype(F32), 64, axis=1)
    return jnp.concatenate([first.astype(BF16), low], axis=1)


def silu(val):
    half = 0.5 * val
    return half + half * jnp.tanh(half)


def layer_kernel(sizes, x_hbm, doc_ref, w_in_hbm, conv_w_ref, conv_b_ref, dt_bias_ref, a_log_ref, d_skip_ref, norm_w_ref, w_out_hbm,
                 out_ref,
                 w_buf, w_bcdt, w_out, x_own, x_t, doc_halo, p_x, p_bc, ho_x, ho_bc, hi_x, hi_bc, par, ub, xs, zs, ys, t_own, s_in, s_out, expand, bias, scores, taps,
                 w_end3, w_start3, a_grp, m_rows, rows_exp, b_t, c_64, sq_sum, normed,
                 w_sems, bc_sem, wo_sems, x_sem, halo_send, halo_recv, misc_send, misc_recv, state_send, state_recv):
    n_tok, d_model, d_inner, conv_dim, n_heads, state_dim, n_seq = sizes
    head_dim = d_inner // n_heads
    n_grp = d_inner // TILE
    per_grp = TILE // head_dim
    n_sub = TILE // LANES
    rank = lax.axis_index('sp')
    has_prev, has_next = rank > 0, rank < n_seq - 1
    lag = (rank // 2) * 3 + rank % 2
    max_lag = ((n_seq - 1) // 2) * 3 + (n_seq - 1) % 2
    conv_width = conv_w_ref.shape[0]

    n_early = 2

    def tile_col(step):
        x_col = d_inner + jnp.where(step == 0, 0, step - n_early) * TILE
        z_col = jnp.where(step <= n_early, step - 1, step - n_grp) * TILE
        is_x = (step == 0) | ((step > n_early) & (step < n_early + n_grp))
        return jnp.where(is_x, x_col, z_col)

    def tile_copy(step):
        slot = lax.rem(step, RING)
        return pltpu.make_async_copy(w_in_hbm.at[pl.ds(pl.multiple_of(tile_col(step), TILE), TILE)], w_buf.at[slot], w_sems.at[slot])

    def tile_start(step):
        @pl.when(step < 2 * n_grp)
        def _():
            tile_copy(step).start()

    def out_copy(step):
        rows = d_inner // n_grp
        return pltpu.make_async_copy(w_out_hbm.at[pl.ds(pl.multiple_of(step * rows, rows), rows)], w_out.at[pl.ds(pl.multiple_of(step * rows, rows), rows)], wo_sems.at[step])

    x_copy = pltpu.make_async_copy(x_hbm, x_own, x_sem)
    bc_copy = pltpu.make_async_copy(w_in_hbm.at[pl.ds(d_inner + d_inner, w_bcdt.shape[0])], w_bcdt, bc_sem)
    x_copy.start()
    bc_copy.start()
    for step in range(RING):
        tile_start(step)

    barrier = pltpu.get_barrier_semaphore()

    @pl.when(has_prev)
    def _():
        pl.semaphore_signal(barrier, inc=1, device_id={'sp': rank - 1}, device_id_type=MESH)

    @pl.when(has_next)
    def _():
        pl.semaphore_signal(barrier, inc=1, device_id={'sp': rank + 1}, device_id_type=MESH)
    pl.semaphore_wait(barrier, has_prev.astype(jnp.int32) + has_next.astype(jnp.int32))

    def to_next(src, dst, send_sem, recv_sem):
        return pltpu.make_async_remote_copy(src_ref=src, dst_ref=dst, send_sem=send_sem, recv_sem=recv_sem, device_id={'sp': rank + 1}, device_id_type=MESH)

    def x_halo(grp):
        return to_next(ho_x.at[grp], hi_x.at[grp], halo_send.at[grp], halo_recv.at[grp])

    def state_copy(grp):
        return to_next(s_out.at[grp], s_in.at[grp], state_send.at[grp], state_recv.at[grp])
    bc_halo = to_next(ho_bc, hi_bc, misc_send.at[0], misc_recv.at[0])
    d_halo = to_next(doc_ref.at[:, pl.ds(n_tok - LANES, LANES)], doc_halo, misc_send.at[1], misc_recv.at[1])

    @pl.when(has_next)
    def _():
        d_halo.start()

    @pl.when(jnp.logical_not(has_prev))
    def _():
        hi_x[...] = jnp.zeros_like(hi_x)
        hi_bc[...] = jnp.zeros_like(hi_bc)
        doc_halo[...] = jnp.zeros_like(doc_halo)
        s_in[...] = jnp.zeros_like(s_in)

    par[...] = jnp.zeros_like(par)
    par[0:1, 0:n_heads] = dt_bias_ref[...]
    par[1:2, 0:n_heads] = a_log_ref[...]
    par[2:3, 0:n_heads] = d_skip_ref[...]
    row_head = iota((4 * n_heads, TILE), 0)
    row_ok = row_head < 3 * n_heads
    row_head = lax.rem(row_head, n_heads)
    lane_head = iota((4 * n_heads, TILE), 1) // head_dim

    def expand_step(grp, carry):
        expand[grp] = jnp.where(row_ok & (row_head == lane_head + grp * per_grp), 1.0, 0.0).astype(BF16)
        return carry
    lax.fori_loop(0, n_grp, expand_step, 0)
    doc_row = doc_ref[...].astype(F32)
    tok_row, tok_lane = iota((n_tok, n_tok), 0), iota((n_tok, n_tok), 1)
    lower = tok_row >= tok_lane
    low_bf = jnp.where(lower, 1.0, 0.0).astype(BF16)
    up_bf = jnp.where(tok_row <= tok_lane, 1.0, 0.0).astype(BF16)
    seg_col = dot(jnp.where(lower, doc_row, 0.0).astype(BF16), jnp.ones((n_tok, n_tok), BF16))
    seg_row = dot(jnp.broadcast_to(doc_row, (8, n_tok)).astype(BF16), up_bf)[0:1]
    bias[...] = jnp.where(lower & (seg_col == seg_row), 0.0, -jnp.inf)

    def project(step):
        slot = lax.rem(step, RING)
        return dot(w_buf[slot], x_t[...]).astype(BF16).T

    def x_project(step, grp):
        tile_copy(step).wait()
        proj = project(step)
        p_x[lax.rem(grp, 2)] = proj
        ho_x[grp] = proj[n_tok - HALO:]
        tile_start(step + RING)

        @pl.when(has_next)
        def _():
            x_halo(grp).start()

    x_copy.wait()
    x_t[...] = x_own[...].T
    bc_copy.wait()
    p_bcdt = dot(w_bcdt[...], x_t[...]).astype(BF16)
    proj_bc = p_bcdt[0:2 * state_dim].T
    p_bc[...] = proj_bc
    ho_bc[...] = proj_bc[n_tok - HALO:]

    @pl.when(has_next)
    def _():
        bc_halo.start()
    x_project(0, 0)

    def early_step(step, carry):
        tile_copy(step).wait()
        zs[step - 1] = project(step)
        tile_start(step + RING)
        return carry
    lax.fori_loop(1, 1 + n_early, early_step, 0)

    @pl.when(has_prev)
    def _():
        bc_halo.wait_recv()
        d_halo.wait_recv()

    doc_ext = jnp.concatenate([doc_halo[...].astype(F32), doc_row], axis=1)
    ext_lane = iota((n_tok + 8, n_tok + LANES), 1)
    ext_ok = (ext_lane >= LANES - 8) & (ext_lane <= iota((n_tok + 8, n_tok + LANES), 0) + (LANES - 8))
    seg_ext = dot(jnp.where(ext_ok, doc_ext, 0.0).astype(BF16), jnp.ones((n_tok + LANES, LANES), BF16))
    for offset in range(1, conv_width):
        taps[offset - 1] = jnp.where(seg_ext[8:] == seg_ext[8 - offset:n_tok + 8 - offset], 1.0, 0.0)

    def conv_lane_tile(proj, halo, col, sub):
        ub[sub, pl.ds(0, 8), :] = halo[HALO - 8:].astype(F32)
        ub[sub, pl.ds(8, n_tok), :] = proj.astype(F32)
        lanes = pl.ds(col, LANES)
        acc = conv_b_ref[:, lanes] + conv_w_ref[0:1, lanes] * ub[sub, pl.ds(8, n_tok), :]
        for offset in range(1, conv_width):
            acc = acc + conv_w_ref[offset:offset + 1, lanes] * (taps[offset - 1] * ub[sub, pl.ds(8 - offset, n_tok), :])
        return silu(acc).astype(BF16)

    bc = conv_lane_tile(p_bc[...], hi_bc[...], d_inner, 0).astype(F32)
    b_t[...] = bc.T[0:state_dim].astype(BF16)
    c_64[...] = pltpu.roll(bc, 64, axis=1)[:, 0:state_dim].astype(BF16)
    scores[...] = dot(c_64[...], b_t[...])
    par_t = par[...].T
    pre_dt = p_bcdt[2 * state_dim:].astype(F32) + par_t[0:n_heads, 0:1]
    dt_val = jnp.maximum(pre_dt, 0.0) + jnp.log1p(jnp.exp(-jnp.abs(pre_dt)))
    log_decay = -jnp.exp(par_t[0:n_heads, 1:2]) * dt_val
    hi, mid, low = split3(log_decay)
    cum = (dot(low, up_bf) + dot(mid, up_bf)) + dot(hi, up_bf)
    cum2 = cum * LOG2E
    m_rows[...] = jnp.log2(dt_val) - cum2
    last_cum, seg_last = cum[:, n_tok - 1:n_tok], seg_row[:, n_tok - 1:n_tok]
    w_end = jnp.where(seg_row == seg_last, jnp.exp(last_cum - cum) * dt_val, 0.0)
    w_start = jnp.where(seg_row == 0.0, jnp.exp(cum), 0.0)
    pad = jnp.zeros((LANES - n_heads, n_tok), F32)
    cum2_col = jnp.concatenate([cum2, pad], axis=0).T
    for grp in range(n_grp):
        a_grp[grp] = pltpu.roll(cum2_col, (LANES - grp * per_grp) % LANES, axis=1)
    w_end3[...] = pack3(jnp.concatenate([w_end, pad], axis=0).T)
    start_col = jnp.concatenate([w_start, pad], axis=0).T
    w_start3[...] = pack3(start_col)
    rows2 = pack3(jnp.concatenate([start_col[n_tok - 1:n_tok], par[2:3, :], jnp.zeros((6, LANES), F32)], axis=0))

    def rows_step(grp, carry):
        rows_exp[grp] = dot(rows2, expand[grp])
        return carry
    lax.fori_loop(0, n_grp, rows_step, 0)

    def serve(slot):
        grp = slot - lag

        @pl.when((grp >= 0) & (grp < n_grp))
        def _():
            @pl.when(has_prev)
            def _():
                state_copy(grp).wait_recv()

            @pl.when(has_next)
            def _():
                s_out[grp] = rows_exp[grp, 0:1, :] * s_in[grp] + t_own[grp]
                state_copy(grp).start()

    def x_step(grp, carry):
        @pl.when(grp < n_grp - 1)
        def _():
            x_project(grp + 1 + n_early, grp + 1)

        @pl.when(has_prev)
        def _():
            x_halo(grp).wait_recv()
        proj, halo = p_x[lax.rem(grp, 2)], hi_x[grp]
        weight = dot(w_end3[...], expand[grp])
        scaled = []
        for sub in range(n_sub):
            xv = conv_lane_tile(proj[:, sub * LANES:(sub + 1) * LANES], halo[:, sub * LANES:(sub + 1) * LANES], pl.multiple_of(grp * TILE + sub * LANES, LANES), sub)
            xs[grp, :, pl.ds(sub * LANES, LANES)] = xv
            scaled.append((xv.astype(F32) * weight[:, sub * LANES:(sub + 1) * LANES]).astype(BF16))
        t_own[grp] = dot(b_t[...], jnp.concatenate(scaled, axis=1))
        serve(grp)
        return carry
    lax.fori_loop(0, n_grp, x_step, 0)

    pair_lane = iota((n_tok, LANES), 1) < head_dim

    def intra(grp):
        a_cols = a_grp[grp]
        m_grp = m_rows[pl.ds(pl.multiple_of(grp * per_grp, per_grp), per_grp), :]
        cb, bs = scores[...], bias[...]
        skip = rows_exp[grp, 1:2, :]
        for pair in range(per_grp // 2):
            lanes = pl.ds(pair * LANES, LANES)
            x_pair = xs[grp, :, lanes]
            mixes = []
            for head in (2 * pair, 2 * pair + 1):
                expo = (a_cols[:, head:head + 1] + m_grp[head:head + 1, :]) + bs
                mixes.append((cb * jnp.exp2(expo)).astype(BF16))
            zero = jnp.zeros_like(x_pair)
            both = jnp.concatenate([jnp.where(pair_lane, x_pair, zero), jnp.where(pair_lane, zero, x_pair)], axis=0)
            ys[grp, :, lanes] = dot(jnp.concatenate(mixes, axis=1), both) + skip[:, pair * LANES:(pair + 1) * LANES] * x_pair.astype(F32)

    def zy_step(grp, carry):
        step = grp + n_grp + n_early
        tile_copy(step).wait()
        zs[grp + n_early] = project(step)
        out_copy(grp).start()
        intra(grp)
        serve(grp + n_grp)
        return carry
    lax.fori_loop(0, n_grp - n_early, zy_step, 0)

    def y_step(grp, carry):
        out_copy(grp).start()
        intra(grp)
        serve(grp + n_grp)
        return carry
    lax.fori_loop(n_grp - n_early, n_grp, y_step, 0)
    for slot in range(2 * n_grp, n_grp + max_lag):
        serve(slot)

    sq_sum[...] = jnp.zeros_like(sq_sum)

    def gate_step(grp, carry):
        from_state = dot(c_64[...], s_in[grp].astype(BF16))
        weight = dot(w_start3[...], expand[grp])
        gated = (ys[grp] + from_state * weight) * silu(zs[grp].astype(F32))
        ys[grp] = gated
        sq = gated * gated
        acc = sq_sum[...]
        for sub in range(n_sub):
            acc = acc + sq[:, sub * LANES:(sub + 1) * LANES]
        sq_sum[...] = acc
        return carry
    lax.fori_loop(0, n_grp, gate_step, 0)

    scale = lax.rsqrt(jnp.sum(sq_sum[...], axis=1, keepdims=True) / d_inner + NORM_EPS)

    def norm_step(grp, carry):
        cols = pl.ds(pl.multiple_of(grp * TILE, TILE), TILE)
        normed[:, cols] = (ys[grp] * scale * norm_w_ref[:, cols]).astype(BF16)
        out_copy(grp).wait()
        return carry
    lax.fori_loop(0, n_grp, norm_step, 0)

    def out_step(col, carry):
        cols = pl.ds(pl.multiple_of(col * TILE, TILE), TILE)
        out_ref[:, cols] = dot(normed[...], w_out[:, cols]).astype(BF16)
        return carry
    lax.fori_loop(0, d_model // TILE, out_step, 0)

    @pl.when(has_next)
    def _():
        d_halo.wait_send()
        bc_halo.wait_send()
        for grp in range(n_grp):
            x_halo(grp).wait_send()
            state_copy(grp).wait_send()


def solution(mesh):
    n_seq = mesh.shape['sp']
    row_spec = P(('dp', 'sp'), None)
    tok_spec = P(('dp', 'sp'))

    def layer_shard(x, doc_start, w_in, conv_w, conv_b, dt_bias, a_log, d_skip, norm_w, w_out):
        n_tok, d_model = x.shape
        d_inner = w_out.shape[0]
        conv_dim = conv_w.shape[1]
        n_heads = a_log.shape[0]
        state_dim = (conv_dim - d_inner) // 2
        n_grp = d_inner // TILE
        sizes = (n_tok, d_model, d_inner, conv_dim, n_heads, state_dim, n_seq)
        vmem = pl.BlockSpec(memory_space=pltpu.VMEM)
        hbm = pl.BlockSpec(memory_space=pl.ANY)
        return pl.pallas_call(
            functools.partial(layer_kernel, sizes),
            out_shape=jax.ShapeDtypeStruct((n_tok, d_model), BF16),
            in_specs=[hbm, vmem, hbm, vmem, vmem, vmem, vmem, vmem, vmem, hbm],
            out_specs=vmem,
            scratch_shapes=[
                pltpu.VMEM((RING, TILE, d_model), BF16),
                pltpu.VMEM((2 * state_dim + n_heads, d_model), BF16),
                pltpu.VMEM((d_inner, d_model), BF16),
                pltpu.VMEM((n_tok, d_model), BF16),
                pltpu.VMEM((d_model, n_tok), BF16),
                pltpu.VMEM((1, LANES), jnp.int32),
                pltpu.VMEM((2, n_tok, TILE), BF16),
                pltpu.VMEM((n_tok, 2 * state_dim), BF16),
                pltpu.VMEM((n_grp, HALO, TILE), BF16),
                pltpu.VMEM((HALO, 2 * state_dim), BF16),
                pltpu.VMEM((n_grp, HALO, TILE), BF16),
                pltpu.VMEM((HALO, 2 * state_dim), BF16),
                pltpu.VMEM((LANES, LANES), F32),
                pltpu.VMEM((TILE // LANES, n_tok + 8, LANES), F32),
                pltpu.VMEM((n_grp, n_tok, TILE), BF16),
                pltpu.VMEM((n_grp, n_tok, TILE), BF16),
                pltpu.VMEM((n_grp, n_tok, TILE), F32),
                pltpu.VMEM((n_grp, state_dim, TILE), F32),
                pltpu.VMEM((n_grp, state_dim, TILE), F32),
                pltpu.VMEM((n_grp, state_dim, TILE), F32),
                pltpu.VMEM((n_grp, 4 * n_heads, TILE), BF16),
                pltpu.VMEM((n_tok, n_tok), F32),
                pltpu.VMEM((n_tok, n_tok), F32),
                pltpu.VMEM((conv_w.shape[0] - 1, n_tok, LANES), F32),
                pltpu.VMEM((n_tok, 2 * LANES), BF16),
                pltpu.VMEM((n_tok, 2 * LANES), BF16),
                pltpu.VMEM((n_grp, n_tok, LANES), F32),
                pltpu.VMEM((n_heads, n_tok), F32),
                pltpu.VMEM((n_grp, 8, TILE), F32),
                pltpu.VMEM((state_dim, n_tok), BF16),
                pltpu.VMEM((n_tok, state_dim), BF16),
                pltpu.VMEM((n_tok, LANES), F32),
                pltpu.VMEM((n_tok, d_inner), BF16),
                pltpu.SemaphoreType.DMA((RING,)),
                pltpu.SemaphoreType.DMA,
                pltpu.SemaphoreType.DMA((n_grp,)),
                pltpu.SemaphoreType.DMA,
                pltpu.SemaphoreType.DMA((n_grp,)),
                pltpu.SemaphoreType.DMA((n_grp,)),
                pltpu.SemaphoreType.DMA((2,)),
                pltpu.SemaphoreType.DMA((2,)),
                pltpu.SemaphoreType.DMA((n_grp,)),
                pltpu.SemaphoreType.DMA((n_grp,)),
            ],
            compiler_params=pltpu.CompilerParams(collective_id=0, has_side_effects=True, vmem_limit_bytes=67043328),
        )(x, doc_start[None, :], w_in.T, conv_w, conv_b[None, :], dt_bias[None, :], a_log[None, :], d_skip[None, :], norm_w, w_out)

    return jax.shard_map(layer_shard, mesh=mesh, in_specs=(row_spec, tok_spec, P(), P(), P(), P(), P(), P(), P(), P()), out_specs=row_spec, check_vma=False)
```
